128 devices in a mesh: row: 8 (over y, core), col: 16 (over x, z).
Axes of the slice: x: 4, y: 4, z: 4, core: 2. Of those that a mesh axis runs over, the one named last changes fastest.
Arguments:
- density: float32 [8192, 65536], P('row', 'col'), may hold values from 0 to 1
- design_mask: int32 [64, 512], P('row', 'col'), may hold values 0 or 1
- rebalance: int32 [32768], replicated, may hold values from 0 to 32767, as said below
Outputs:
- balanced: bfloat16 [32768, 128, 128], P(('row', 'col'))
- constraint: float32 [], replicated
The draws below stay inside these ranges and needn't reach their ends.
Inputs may be any that keep to these rules, and one draw needn't show every extreme that they name: `rebalance`: A permutation of the 32768 block numbers. Of the blocks that one device holds, the ones that land among one device's output blocks number exactly 2 or none.
All inputs are finite; a program needn't handle non-finite values. No bound on the sum of `design_mask` on one device may be relied on, other than what follows from the above.
Results may differ from the reference program's by a relative error of at most 0.001.
Values may be sent and summed in bfloat16 or wider, within the bound.
A program may use at most 192 MiB of HBM per device.

```python
import jax
import jax.numpy as jnp
from jax import lax

BS = 128
RADIUS = 16
KR = 8
KC = 32
BLOCKS_DEV = 256
CAP = 2
NX = 8192
NY = 65536
NBLK = 32768
N_ROW = 8
N_COL = 16


def draw_rebalance(key, part):
    device_count = N_ROW * N_COL
    group_count = BLOCKS_DEV // CAP
    base = jax.random.fold_in(key, 11)
    key_order, key_offset, key_source, key_target = jax.random.split(base, 4)
    order = jax.random.permutation(key_order, device_count).astype(jnp.int32)
    inverse = jnp.argsort(order).astype(jnp.int32)
    offsets = jax.random.permutation(key_offset, device_count)[:group_count].astype(jnp.int32)
    source_shuffle = jax.vmap(lambda sub: jax.random.permutation(sub, BLOCKS_DEV))(jax.random.split(key_source, device_count)).astype(jnp.int32)
    target_shuffle = jax.vmap(lambda sub: jax.random.permutation(sub, BLOCKS_DEV))(jax.random.split(key_target, device_count)).astype(jnp.int32)
    positions = jnp.arange(NBLK, dtype=jnp.int32)
    target_dev = positions // BLOCKS_DEV
    target_slot = positions % BLOCKS_DEV
    raw_slot = target_shuffle[target_dev, target_slot]
    group = raw_slot // CAP
    within = raw_slot % CAP
    source_dev = (inverse[target_dev] - offsets[group]) % device_count
    local_block = source_shuffle[source_dev, group * CAP + within]
    source_row = source_dev // N_COL
    source_col = source_dev % N_COL
    block_row = source_row * KR + local_block // KC
    block_col = source_col * KC + local_block % KC
    return (block_row * (KC * N_COL) + block_col).astype(jnp.int32)


def set_ends(entries, own_key, smallest, largest):
    place = [jax.random.randint(jax.random.fold_in(own_key, axis), (), 0, length) for axis, length in enumerate(entries.shape)]
    longest = entries.shape.index(max(entries.shape))
    next_to = place[:longest] + [(place[longest] + 1) % entries.shape[longest]] + place[longest + 1:]
    return entries.at[tuple(place)].set(smallest).at[tuple(next_to)].set(largest)


def levels(key, shape, cuts, smallest, high):
    factor_of = 1.0
    for axis_at, shards_of in cuts:
        heights = jax.random.uniform(jax.random.fold_in(jax.random.fold_in(key, 6), axis_at), (shards_of,), jnp.float32, smallest / len(cuts), high / len(cuts))
        factor_of = factor_of * jnp.repeat(jnp.exp(heights), shape[axis_at] // shards_of).reshape((-1,) + (1,) * (len(shape) - 1 - axis_at))
    return factor_of


def setup_inputs(seed: int = 0) -> dict:
    key_list = jax.random.split(jax.random.key(seed), 4)
    return {
        "density": jnp.clip(1.0 * jax.random.uniform(key_list[0], (NX, NY), jnp.float32) ** levels(key_list[0], (NX, NY), ((0, 8), (1, 16)), -0.2, 0.2), 0.0, 1.0),
        "design_mask": set_ends((jax.random.randint(key_list[1], (NX // BS, NY // BS), 0, 4) < 3).astype(jnp.int32), jax.random.fold_in(key_list[1], 1), 0, 1),
        "rebalance": draw_rebalance(jax.random.fold_in(key_list[3], 71), 0),
    }


SHARPNESS = 32.0
THRESHOLD = 0.5
VOLUME_TARGET = 0.4


def filter_taps():
    sigma = RADIUS / 4.0
    offsets = jnp.arange(2 * RADIUS + 1, dtype=jnp.float32) - RADIUS
    raw_taps = jnp.exp(-offsets * offsets / (2.0 * sigma * sigma))
    return raw_taps / jnp.sum(raw_taps)


def smooth(field, weights, axis):
    length = field.shape[axis]
    widths = [(0, 0), (0, 0)]
    widths[axis] = (RADIUS, RADIUS)
    padded = jnp.pad(field, widths)
    total = jnp.zeros_like(field)
    for offset in range(2 * RADIUS + 1):
        total = total + weights[offset] * lax.slice_in_dim(padded, offset, offset + length, axis=axis)
    return total


def reference(density, design_mask, rebalance):
    weights = filter_taps()
    along_rows = smooth(density, weights, 0)
    filtered = smooth(along_rows, weights, 1)
    cell_mask = jnp.repeat(jnp.repeat(design_mask, BS, 0), BS, 1).astype(jnp.float32)
    lower = jnp.tanh(SHARPNESS * THRESHOLD)
    upper = jnp.tanh(SHARPNESS * (1.0 - THRESHOLD))
    projected = cell_mask * (lower + jnp.tanh(SHARPNESS * (filtered - THRESHOLD))) / (lower + upper)
    constraint = jnp.sum(projected) / (NX * NY) / VOLUME_TARGET - 1.0
    block_rows = NX // BS
    block_cols = NY // BS
    tiles = projected.astype(jnp.bfloat16).reshape(block_rows, BS, block_cols, BS)
    tiles = tiles.transpose(0, 2, 1, 3).reshape(block_rows * block_cols, BS, BS)
    balanced = jnp.take(tiles, rebalance.astype(jnp.int32), axis=0)
    return balanced, constraint
```

```python
import functools

import jax
import jax.numpy as jnp
import numpy as np
from jax import lax
from jax.experimental import pallas as pl
from jax.experimental.pallas import tpu as pltpu
from jax.sharding import PartitionSpec as P

BS = 128
RADIUS = 16
SHARPNESS = 32.0
THRESHOLD = 0.5
VOLUME_TARGET = 0.4
MESH = pl.DeviceIdType.MESH

KR = 8
KC = 32
SIDE = 4
GROUPS = 4
WIN = BS + 2 * RADIUS
ROWS = KR * BS
COLS = KC * BS
UNROLL = 8

ROUTES = ((0, 1, 2), (1, 2, 0), (2, 0, 1))
PARTS = ((0, 48), (48, 48), (96, 32))
CHUNKS = tuple(
    (g, g % 2, ROUTES[i], *PARTS[(i + g) % 3]) for g in range(GROUPS) for i in range(3)
)
NCH = len(CHUNKS)


def filter_taps():
    sigma = RADIUS / 4.0
    offsets = np.arange(2 * RADIUS + 1, dtype=np.float64) - RADIUS
    raw = np.exp(-offsets * offsets / (2.0 * sigma * sigma))
    return raw / raw.sum()


def taps_at(lag):
    taps = filter_taps()
    inside = (lag >= 0) & (lag <= 2 * RADIUS)
    return np.where(inside, taps[np.clip(lag, 0, 2 * RADIUS)], 0.0).astype(np.float32)


def high_low(array):
    high = array.astype(jnp.bfloat16)
    low = (array - high.astype(np.float32)).astype(jnp.bfloat16)
    return high, low


def row_weights():
    lag = np.arange(WIN)[None, :] - np.arange(BS)[:, None]
    return np.concatenate(high_low(taps_at(lag)), axis=0)


def col_weights():
    lane = np.arange(BS)
    edge = np.where(lane < BS // 2, lane + BS, lane - BS)
    position = np.concatenate([lane, edge])
    lag = position[:, None] - lane[None, :] + RADIUS
    once = np.concatenate(high_low(taps_at(lag)), axis=1)
    return np.concatenate([once, once], axis=0)


def split_f32(value):
    high = value.astype(jnp.bfloat16)
    low = (value - high.astype(jnp.float32)).astype(jnp.bfloat16)
    return high, low


def fused_kernel(
    density, table, mask, w_row, w_col,
    arrived, total,
    win_top, win_bot, win, a_hi, a_lo, send, mid1, mid2, edge_out, edge_in, sums,
    load_sem, halo_send, halo_recv, edge_send, edge_recv, sum_send, sum_recv,
    out_send, out_recv, local_sem,
):
    row = lax.axis_index("row")
    col = lax.axis_index("col")
    y, core = row // 2, row % 2
    x, z = col // SIDE, col % SIDE
    me = (x, y, z)

    def device(c, k):
        return (c[1] * 2 + k, c[0] * SIDE + c[2])

    def along(axis, step):
        c = list(me)
        c[axis] = lax.rem(me[axis] + step, SIDE)
        return c

    def load(i, slot):
        return pltpu.make_async_copy(
            density.at[pl.ds(i * BS - RADIUS, WIN)], win.at[slot], load_sem.at[slot]
        )

    top_load = pltpu.make_async_copy(
        density.at[pl.ds(0, BS + RADIUS)], win_top.at[pl.ds(RADIUS, BS + RADIUS)], load_sem.at[2]
    )
    bot_load = pltpu.make_async_copy(
        density.at[pl.ds(ROWS - BS - RADIUS, BS + RADIUS)],
        win_bot.at[pl.ds(0, BS + RADIUS)],
        load_sem.at[3],
    )
    load(1, 0).start()
    load(2, 1).start()
    top_load.start()
    bot_load.start()

    row_next, row_prev = lax.rem(row + 1, 8), lax.rem(row + 7, 8)
    col_next, col_prev = lax.rem(col + 1, 16), lax.rem(col + 15, 16)
    barrier = pltpu.get_barrier_semaphore()
    count = 0
    for axis in range(3):
        for step in range(1, SIDE):
            for k in range(2):
                pl.semaphore_signal(
                    barrier, inc=1, device_id=device(along(axis, step), lax.rem(core + k, 2)),
                    device_id_type=MESH,
                )
                count += 1
    for target in (device(me, 1 - core), (row, col_next), (row, col_prev)):
        pl.semaphore_signal(barrier, inc=1, device_id=target, device_id_type=MESH)
        count += 1
    pl.semaphore_wait(barrier, count)

    down = pltpu.make_async_remote_copy(
        src_ref=density.at[pl.ds(ROWS - RADIUS, RADIUS)], dst_ref=win_top.at[pl.ds(0, RADIUS)],
        send_sem=halo_send.at[0], recv_sem=halo_recv.at[0],
        device_id=(row_next, col), device_id_type=MESH,
    )
    up = pltpu.make_async_remote_copy(
        src_ref=density.at[pl.ds(0, RADIUS)], dst_ref=win_bot.at[pl.ds(BS + RADIUS, RADIUS)],
        send_sem=halo_send.at[1], recv_sem=halo_recv.at[1],
        device_id=(row_prev, col), device_id_type=MESH,
    )
    down.start()
    up.start()

    taps_row = w_row[...]

    def first(window, i, tile):
        value = window[:, pl.ds(pl.multiple_of(tile * BS, BS), BS)]
        high, low = split_f32(value)
        got = jnp.dot(
            taps_row, jnp.concatenate([high, low], axis=1), preferred_element_type=jnp.float32
        )
        part = got[:BS] + got[BS:]
        value = part[:, :BS] + part[:, BS:]
        high, low = split_f32(value)
        a_hi[i, tile + 1] = high
        a_lo[i, tile + 1] = low
        return value

    def edges(i, left, right):
        lane = lax.broadcasted_iota(jnp.int32, (BS, BS), 1) // RADIUS == i
        for side, (tile, first_lane) in enumerate(((left, 0), (right, BS - RADIUS))):
            moved = pltpu.roll(tile, (RADIUS * i - first_lane) % BS, 1)
            edge_out[side] = jnp.where(lane, moved, edge_out[side])

    edge_out[...] = jnp.zeros_like(edge_out)

    def tiles(window, i, begin, end):
        def body(step, carry):
            for u in range(UNROLL):
                first(window, i, begin + step * UNROLL + u)
            return carry

        lax.fori_loop(0, (end - begin) // UNROLL, body, 0)

    def whole_row(window, i):
        tiles(window, i, 0, KC)

    def edge_tile(i, tile):
        return a_hi[i, tile + 1].astype(jnp.float32) + a_lo[i, tile + 1].astype(jnp.float32)

    for i in range(1, KR - 1):
        slot = (i - 1) % 2
        load(i, slot).wait()
        whole_row(win.at[slot], i)
        edges(i, edge_tile(i, 0), edge_tile(i, KC - 1))
        if i + 2 < KR - 1:
            load(i + 2, slot).start()

    top_load.wait()
    down.wait_recv()
    keep = jnp.where(row > 0, 1.0, 0.0).astype(jnp.float32)
    win_top[pl.ds(0, RADIUS), :] = win_top[pl.ds(0, RADIUS), :] * keep
    whole_row(win_top, 0)
    edges(0, edge_tile(0, 0), edge_tile(0, KC - 1))
    bot_load.wait()
    up.wait_recv()
    keep = jnp.where(row < 7, 1.0, 0.0).astype(jnp.float32)
    win_bot[pl.ds(BS + RADIUS, RADIUS), :] = win_bot[pl.ds(BS + RADIUS, RADIUS), :] * keep
    whole_row(win_bot, KR - 1)
    edges(KR - 1, edge_tile(KR - 1, 0), edge_tile(KR - 1, KC - 1))

    to_left = pltpu.make_async_remote_copy(
        src_ref=edge_out.at[0], dst_ref=edge_in.at[1],
        send_sem=edge_send.at[0], recv_sem=edge_recv.at[1],
        device_id=(row, col_prev), device_id_type=MESH,
    )
    to_right = pltpu.make_async_remote_copy(
        src_ref=edge_out.at[1], dst_ref=edge_in.at[0],
        send_sem=edge_send.at[1], recv_sem=edge_recv.at[0],
        device_id=(row, col_next), device_id_type=MESH,
    )
    to_left.start()
    to_right.start()
    to_right.wait_recv()
    to_left.wait_recv()
    for side, (inside, tile, first_lane) in enumerate(
        ((col > 0, 0, BS - RADIUS), (col < 15, KC + 1, 0))
    ):
        value = edge_in[side] * jnp.where(inside, 1.0, 0.0).astype(jnp.float32)
        high, low = split_f32(value)
        high, low = high.astype(jnp.float32), low.astype(jnp.float32)
        for i in range(KR):
            shift = (first_lane - RADIUS * i) % BS
            a_hi[i, tile] = pltpu.roll(high, shift, 1).astype(jnp.bfloat16)
            a_lo[i, tile] = pltpu.roll(low, shift, 1).astype(jnp.bfloat16)

    right_half = lax.broadcasted_iota(jnp.int32, (BS, BS), 1) < BS // 2
    lower = float(np.tanh(np.float32(SHARPNESS * THRESHOLD)))
    upper = float(np.tanh(np.float32(SHARPNESS * (1.0 - THRESHOLD))))

    def second(block):
        i = block // KC
        tile = lax.rem(block, KC)
        pieces = []
        for ref in (a_hi, a_lo):
            pieces.append(ref[i, tile + 1])
            pieces.append(jnp.where(right_half, ref[i, tile + 2], ref[i, tile]))
        got = jnp.dot(
            jnp.concatenate(pieces, axis=1), w_col[...], preferred_element_type=jnp.float32
        )
        filtered = got[:, :BS] + got[:, BS:]
        scale = mask[block].astype(jnp.float32) * (1.0 / (lower + upper))
        return scale * (lower + jnp.tanh(SHARPNESS * (filtered - THRESHOLD)))

    def view(ref, g, picks, begin, rows):
        index = [picks.get(d, slice(None)) for d in range(3)]
        return ref.at[(g, *index, pl.ds(begin, rows), slice(None))]

    def remote(src, dst, axis, step, flip, sem):
        pltpu.make_async_remote_copy(
            src_ref=src, dst_ref=dst, send_sem=out_send.at[sem], recv_sem=out_recv.at[sem],
            device_id=device(along(axis, step), lax.rem(core + flip, 2)), device_id_type=MESH,
        ).start()

    def wait(sem, ref):
        pltpu.make_async_copy(ref, ref, sem).wait()

    others = pl.ds(1, SIDE - 1)
    steps = (1, 3, 2)

    def hop1(j):
        g, flip, (a, b, c), begin, rows = CHUNKS[j]
        for step in ((0,) if flip else ()) + steps:
            remote(
                view(send, g, {a: step}, begin, rows), view(mid1, g, {a: step}, begin, rows),
                a, step, flip, j,
            )

    def got1(j):
        g, flip, (a, b, c), begin, rows = CHUNKS[j]
        return view(mid1, g, {} if flip else {a: others}, begin, rows)

    def hop2(j):
        g, flip, (a, b, c), begin, rows = CHUNKS[j]
        wait(out_recv.at[j], got1(j))
        for step in steps:
            if flip:
                pairs = ((mid1, {b: step}),)
            else:
                pairs = ((mid1, {b: step, a: others}), (send, {b: step, a: 0}))
            for ref, picks in pairs:
                remote(
                    view(ref, g, picks, begin, rows), view(mid2, g, picks, begin, rows),
                    b, step, 0, NCH + j,
                )

    def got2(j):
        g, flip, (a, b, c), begin, rows = CHUNKS[j]
        return view(mid2, g, {b: others}, begin, rows)

    def hop3(j):
        g, flip, (a, b, c), begin, rows = CHUNKS[j]
        wait(out_recv.at[NCH + j], got2(j))
        for step in steps + (0,):
            pairs = [(mid2, {c: step, b: others})]
            if flip:
                pairs.append((mid1, {c: step, b: 0}))
            else:
                pairs.append((mid1, {c: step, b: 0, a: others}))
                pairs.append((send, {c: step, b: 0, a: 0}))
            for ref, picks in pairs:
                src, dst = view(ref, g, picks, begin, rows), view(arrived, g, picks, begin, rows)
                if step:
                    remote(src, dst, c, step, 0, 2 * NCH + j)
                else:
                    pltpu.make_async_copy(src, dst, local_sem.at[0]).start()

    def got3(j):
        g, flip, (a, b, c), begin, rows = CHUNKS[j]
        return view(arrived, g, {c: others}, begin, rows)

    volume = jnp.zeros((8, BS), jnp.float32)
    for g in range(GROUPS):

        def body(step, acc, g=g):
            dx = step // 2
            for u in range(UNROLL):
                dy, dz = lax.rem(step, 2) * 2 + u // SIDE, u % SIDE
                target_row = lax.rem(y + dy, SIDE) * 2 + lax.rem(core + g, 2)
                target_col = lax.rem(x + dx, SIDE) * SIDE + (z + dz) % SIDE
                target = target_row * 16 + target_col
                block = table[target * 2 + g // 2]
                value = second(block)
                send[g, dx, dy, dz] = value.astype(jnp.bfloat16)
                acc = acc + jnp.sum(value.reshape(BS // 8, 8, BS), axis=0)
            return acc

        volume = lax.fori_loop(0, 64 // UNROLL, body, volume)
        for j in range(3 * g, 3 * g + 3):
            hop1(j)

    def spread(stage, own, slots, targets):
        first_slot = (0, 8, 12)[stage]
        sums[first_slot + own] = volume_parts[stage]
        for target in targets:
            pltpu.make_async_remote_copy(
                src_ref=sums.at[first_slot + own], dst_ref=sums.at[first_slot + own],
                send_sem=sum_send.at[stage], recv_sem=sum_recv.at[stage],
                device_id=target, device_id_type=MESH,
            ).start()

    def collect(stage, slots):
        first_slot = (0, 8, 12)[stage]
        for sem in (sum_recv, sum_send):
            wait(sem.at[stage], sums.at[pl.ds(first_slot, slots - 1)])
        out = sums[first_slot]
        for s in range(1, slots):
            out = out + sums[first_slot + s]
        return out

    volume_parts = [volume]
    spread(
        0, x * 2 + core, 8,
        [device(along(0, s), lax.rem(core + k, 2)) for s in range(SIDE) for k in range(2) if s or k],
    )
    for j in range(NCH):
        hop2(j)
    volume_parts.append(collect(0, 8))
    spread(1, y, 4, [device(along(1, s), core) for s in range(1, SIDE)])
    for j in range(NCH):
        hop3(j)
    volume_parts.append(collect(1, 4))
    spread(2, z, 4, [device(along(2, s), core) for s in range(1, SIDE)])
    all_volume = jnp.sum(collect(2, 4))
    cells = float(ROWS * COLS * 128)
    constraint = all_volume / cells / VOLUME_TARGET - 1.0
    total[...] = jnp.full((8, BS), constraint, jnp.float32)

    for j in range(NCH):
        wait(out_recv.at[2 * NCH + j], got3(j))
    for j in range(NCH):
        wait(out_send.at[j], got1(j))
        wait(out_send.at[NCH + j], got2(j))
        wait(out_send.at[2 * NCH + j], got3(j))
        g, flip, (a, b, c), begin, rows = CHUNKS[j]
        wait(local_sem.at[0], view(arrived, g, {c: 0}, begin, rows))
    for copy in (down, up, to_left, to_right):
        copy.wait_send()


def place_kernel(index, arrived, out, held, in_sem, out_sem):
    parts = 8
    per = KR * KC // parts

    def start(j, carry):
        pltpu.make_async_copy(arrived.at[index[j]], held.at[j], in_sem.at[j // per]).start()
        return carry

    lax.fori_loop(0, KR * KC, start, 0, unroll=8)
    for p in range(parts):
        piece = pl.ds(p * per, per)
        pltpu.make_async_copy(arrived.at[piece], held.at[piece], in_sem.at[p]).wait()
        pltpu.make_async_copy(held.at[piece], out.at[piece], out_sem.at[p]).start()
    for p in range(parts):
        piece = pl.ds(p * per, per)
        pltpu.make_async_copy(held.at[piece], out.at[piece], out_sem.at[p]).wait()


def tables(rebalance):
    row, col = lax.axis_index("row"), lax.axis_index("col")
    ids = rebalance.reshape(128, KR * KC)

    def owner(ids):
        block_row, block_col = ids // (KC * 16), ids % (KC * 16)
        device = block_row // KR * 16 + block_col // KC
        return device, block_row % KR * KC + block_col % KC

    device, local = owner(ids)
    me = row * 16 + col
    mine = device == me
    low = jnp.min(jnp.where(mine, local, 1 << 20), axis=1)
    high = jnp.max(jnp.where(mine, local, -1), axis=1)
    table = jnp.stack([low, high], axis=1).reshape(-1)

    own = lax.dynamic_slice_in_dim(ids, me, 1, 0)[0]
    source, block = owner(own)
    earlier = (source[:, None] == source[None, :]) & (block[None, :] < block[:, None])
    rank = jnp.sum(earlier.astype(jnp.int32), axis=1)
    source_row, source_col = source // 16, source % 16
    dy = (row // 2 - source_row // 2) % SIDE
    flip = (row + source_row) % 2
    dx = (col // SIDE - source_col // SIDE) % SIDE
    dz = (col - source_col) % SIDE
    index = (rank * 2 + flip) * 64 + dx * 16 + dy * SIDE + dz
    return table, index


def per_device(density, design_mask, rebalance):
    table, index = tables(rebalance)
    smem = pl.BlockSpec(memory_space=pltpu.SMEM)
    vmem = pl.BlockSpec(memory_space=pltpu.VMEM)
    anywhere = pl.BlockSpec(memory_space=pl.ANY)
    exchange = (GROUPS, SIDE, SIDE, SIDE, BS, BS)
    window = pltpu.VMEM((WIN, COLS), jnp.float32)
    field = pltpu.VMEM((KR, KC + 2, BS, BS), jnp.bfloat16)
    dma = pltpu.SemaphoreType.DMA
    arrived, total = pl.pallas_call(
        fused_kernel,
        out_shape=(
            jax.ShapeDtypeStruct(exchange, jnp.bfloat16),
            jax.ShapeDtypeStruct((8, BS), jnp.float32),
        ),
        in_specs=[anywhere, smem, smem, vmem, vmem],
        out_specs=(anywhere, vmem),
        scratch_shapes=[
            window, window, pltpu.VMEM((2, WIN, COLS), jnp.float32), field, field,
            *[pltpu.VMEM(exchange, jnp.bfloat16)] * 3,
            pltpu.VMEM((2, BS, BS), jnp.float32), pltpu.VMEM((2, BS, BS), jnp.float32),
            pltpu.VMEM((16, 8, BS), jnp.float32),
            dma((4,)), dma((2,)), dma((2,)), dma((2,)), dma((2,)), dma((3,)), dma((3,)),
            dma((3 * NCH,)), dma((3 * NCH,)), dma((1,)),
        ],
        compiler_params=pltpu.CompilerParams(
            collective_id=0, has_side_effects=True, vmem_limit_bytes=63 * 2**20
        ),
        name="filter_exchange",
    )(
        density, table, design_mask.reshape(-1),
        jnp.asarray(row_weights()), jnp.asarray(col_weights()),
    )
    balanced = pl.pallas_call(
        place_kernel,
        out_shape=jax.ShapeDtypeStruct((KR * KC, BS, BS), jnp.bfloat16),
        in_specs=[smem, anywhere],
        out_specs=anywhere,
        scratch_shapes=[pltpu.VMEM((KR * KC, BS, BS), jnp.bfloat16), dma((8,)), dma((8,))],
        compiler_params=pltpu.CompilerParams(vmem_limit_bytes=16 * 2**20),
        name="place_blocks",
    )(index, arrived.reshape(KR * KC, BS, BS))
    return balanced, total[0, 0]


def solution(mesh):
    return jax.shard_map(
        per_device, mesh=mesh,
        in_specs=(P("row", "col"), P("row", "col"), P()),
        out_specs=(P(("row", "col"), None, None), P()),
        check_vma=False,
    )
```

```python
import functools

import jax
import jax.numpy as jnp
import numpy as np
from jax import lax
from jax.experimental import pallas as pl
from jax.experimental.pallas import tpu as pltpu
from jax.sharding import PartitionSpec as P

BS = 128
RADIUS = 16
SHARPNESS = 32.0
THRESHOLD = 0.5
VOLUME_TARGET = 0.4
MESH = pl.DeviceIdType.MESH

KR = 8
KC = 32
SIDE = 4
GROUPS = 4
WIN = BS + 2 * RADIUS
ROWS = KR * BS
COLS = KC * BS
GROUPS_IN = ROWS // RADIUS
BATCH = 16
PACK = 4
STEPS = (1, 3, 2, 0)
OTHERS = pl.ds(0, SIDE - 1)
HOME = SIDE - 1

ROUTES = ((0, 1, 2), (1, 2, 0), (2, 0, 1))
PARTS = ((0, 48), (48, 48), (96, 32))
CHUNKS = tuple(
    (g, g % 2, ROUTES[i], *PARTS[(i + g) % 3]) for g in range(GROUPS) for i in range(3)
)
NCH = len(CHUNKS)


def filter_taps():
    sigma = RADIUS / 4.0
    offsets = np.arange(2 * RADIUS + 1, dtype=np.float64) - RADIUS
    raw = np.exp(-offsets * offsets / (2.0 * sigma * sigma))
    return raw / raw.sum()


def taps_at(lag):
    taps = filter_taps()
    inside = (lag >= 0) & (lag <= 2 * RADIUS)
    return np.where(inside, taps[np.clip(lag, 0, 2 * RADIUS)], 0.0).astype(np.float32)


def high_low(array):
    high = array.astype(jnp.bfloat16)
    low = (array - high.astype(np.float32)).astype(jnp.bfloat16)
    return high, low


def row_weights():
    lag = np.arange(WIN)[None, :] - np.arange(BS)[:, None]
    once = np.concatenate(high_low(taps_at(lag)), axis=0)
    return np.concatenate([once, once], axis=1)


def col_weights():
    lane = np.arange(BS)
    edge = np.where(lane < BS // 2, lane + BS, lane - BS)
    position = np.concatenate([lane, edge])
    lag = position[:, None] - lane[None, :] + RADIUS
    once = np.concatenate(high_low(taps_at(lag)), axis=1)
    return np.concatenate([once, once], axis=0)


def split_f32(value):
    high = value.astype(jnp.bfloat16)
    low = (value - high.astype(jnp.float32)).astype(jnp.bfloat16)
    return high, low


def fused_kernel(
    density, rebalance, w_row_in, w_col_in, mask,
    arrived, slots, total,
    field, rim, along_rows, ids, w_row, w_col, keys, table, send, mid1, mid2, edge_out, edge_in, sums,
    load_sem, aux_sem, table_sem, halo_send, halo_recv, sum_send, sum_recv,
    out_send, out_recv, local_sem,
):
    row = lax.axis_index("row")
    col = lax.axis_index("col")
    y, core = row // 2, row % 2
    x, z = col // SIDE, col % SIDE
    me = (x, y, z)
    my_id = row * 16 + col

    def device(c, k):
        return (c[1] * 2 + k, c[0] * SIDE + c[2])

    def along(axis, step):
        c = list(me)
        c[axis] = lax.rem(me[axis] + step, SIDE)
        return c

    inner = pl.ds(1, GROUPS_IN)
    aux = [
        pltpu.make_async_copy(src, dst, aux_sem.at[n])
        for n, (src, dst) in enumerate(((rebalance, ids), (w_row_in, w_row), (w_col_in, w_col)))
    ]
    loads = [
        pltpu.make_async_copy(
            density.at[:, :, pl.ds(tile * BS, BS)], field.at[tile + 1, inner], load_sem.at[n]
        )
        for n, tile in enumerate((0, KC - 1, *range(1, KC - 1)))
    ]
    edge_loads, loads = loads[:2], loads[2:]
    for copy in (*edge_loads, *aux, *loads):
        copy.start()

    next_row, prev_row = lax.rem(row + 1, 8), lax.rem(row + 7, 8)
    next_col, prev_col = lax.rem(col + 1, 16), lax.rem(col + 15, 16)
    greeted = [
        device(along(axis, step), lax.rem(core + k, 2))
        for axis in range(3) for step in range(1, SIDE) for k in range(2)
    ]
    greeted += [device(me, 1 - core), (row, next_col), (row, prev_col)]
    greeted += [(r, c) for r in (next_row, prev_row) for c in (next_col, prev_col)]
    barrier = pltpu.get_barrier_semaphore()
    for target in greeted:
        pl.semaphore_signal(barrier, inc=1, device_id=target, device_id_type=MESH)

    for copy in edge_loads:
        copy.wait()
    lane_group = lax.broadcasted_iota(jnp.int32, (BS, BS), 1) // RADIUS
    for side, (tile, first_lane) in enumerate(((0, 0), (KC - 1, BS - RADIUS))):
        packed = jnp.zeros((BS, BS), jnp.float32)
        for i in range(KR):
            value = field[tile + 1, pl.ds(1 + i * 8, 8)].reshape(BS, BS)
            moved = pltpu.roll(value, (RADIUS * i - first_lane) % BS, 1)
            packed = jnp.where(lane_group == i, moved, packed)
        edge_out[side] = packed

    pl.semaphore_wait(barrier, len(greeted))

    last = GROUPS_IN - 1
    own_left, own_right = pl.ds(0, BS), pl.ds(COLS - BS, BS)
    wide, left, right = pl.ds(BS, COLS), pl.ds(0, BS), pl.ds(BS + COLS, BS)
    halo = [
        (edge_out.at[0], edge_in.at[1], (row, prev_col)),
        (edge_out.at[1], edge_in.at[0], (row, next_col)),
        (density.at[last], rim.at[0, :, wide], (next_row, col)),
        (density.at[0], rim.at[1, :, wide], (prev_row, col)),
        (density.at[last, :, own_right], rim.at[0, :, left], (next_row, next_col)),
        (density.at[last, :, own_left], rim.at[0, :, right], (next_row, prev_col)),
        (density.at[0, :, own_right], rim.at[1, :, left], (prev_row, next_col)),
        (density.at[0, :, own_left], rim.at[1, :, right], (prev_row, prev_col)),
    ]
    halo = [
        pltpu.make_async_remote_copy(
            src_ref=src, dst_ref=dst, send_sem=halo_send.at[n], recv_sem=halo_recv.at[n],
            device_id=target, device_id_type=MESH,
        )
        for n, (src, dst, target) in enumerate(halo)
    ]
    for copy in halo:
        copy.start()

    for copy in aux:
        copy.wait()

    def owner(number):
        return (number >> 12) * 16 + ((number >> 5) & 15)

    def local(number):
        return ((number >> 9) & 7) * KC + (number & (KC - 1))

    none = 1 << 20
    turned = ids[...].T
    mine = owner(turned) == my_id
    block = local(turned)
    keys[pl.ds(0, 1), :] = jnp.min(jnp.where(mine, block, none), 0, keepdims=True)
    keys[pl.ds(1, 1), :] = jnp.max(jnp.where(mine, block, -1), 0, keepdims=True)
    to_table = pltpu.make_async_copy(keys, table, table_sem.at[0])
    to_table.start()
    low, high = jnp.full((1, BS), none, jnp.int32), jnp.full((1, BS), -1, jnp.int32)
    source = lax.broadcasted_iota(jnp.int32, (BS, BS), 1)
    for half in range(2):
        own = jnp.broadcast_to(ids[pl.ds(my_id * 2 + half, 1), :], (BS, BS)).T
        slot = lax.broadcasted_iota(jnp.int32, (BS, BS), 0) + half * BS
        key = local(own) * 256 + slot
        here = owner(own) == source
        low = jnp.minimum(low, jnp.min(jnp.where(here, key, none), 0, keepdims=True))
        high = jnp.maximum(high, jnp.max(jnp.where(here, key, -1), 0, keepdims=True))
    slots[...] = jnp.zeros_like(slots)
    slots[pl.ds(0, 1), :] = low & 255
    slots[pl.ds(1, 1), :] = high & 255

    for copy in halo:
        copy.wait_recv()
    for copy in loads:
        copy.wait()

    def kept(condition):
        return jnp.where(condition, 1.0, 0.0).astype(jnp.float32)

    keep_side = (kept(col > 0), kept(col < 15))
    for side, (tile, first_lane) in enumerate(((0, BS - RADIUS), (KC + 1, 0))):
        value = edge_in[side] * keep_side[side]
        for i in range(KR):
            moved = pltpu.roll(value, (first_lane - RADIUS * i) % BS, 1)
            field[tile, pl.ds(1 + i * 8, 8)] = moved.reshape(8, RADIUS, BS)
    for end, (group, keep) in enumerate(((0, kept(row > 0)), (GROUPS_IN + 1, kept(row < 7)))):
        for tile in range(KC + 2):
            scale = keep * keep_side[tile > 0] if tile in (0, KC + 1) else keep
            field[tile, group] = rim[end, :, tile * BS : (tile + 1) * BS] * scale
    to_table.wait()

    right_half = lax.broadcasted_iota(jnp.int32, (WIN, BS), 1) < BS // 2
    quarter = lax.broadcasted_iota(jnp.int32, (WIN, BS), 1) // (2 * RADIUS)
    lower = float(np.tanh(np.float32(SHARPNESS * THRESHOLD)))
    upper = float(np.tanh(np.float32(SHARPNESS * (1.0 - THRESHOLD))))

    def turn(n):
        return 2 * RADIUS * n + RADIUS

    def first_filter(tiles, uses):
        window = jnp.concatenate(tiles, axis=1)
        got = jnp.dot(
            w_row[...], jnp.concatenate(split_f32(window), axis=0),
            preferred_element_type=jnp.float32,
        )
        got = got[:BS] + got[BS:]
        for n, tile_uses in enumerate(uses):
            for u, offset, shift in tile_uses:
                value = got[:, n * BS : (n + 1) * BS]
                if shift:
                    value = pltpu.roll(value, shift, 1)
                for m, piece in enumerate(split_f32(value)):
                    at = 2 * BS * m + offset
                    along_rows[u * BS : (u + 1) * BS, at : at + BS] = piece

    def batch(blocks):
        waiting = []
        packed = None
        for u, block in enumerate(blocks):
            tile = block & (KC - 1)
            group = (block >> 5) * 8

            def part(offset):
                return jnp.concatenate(
                    [field[tile + offset, group + n] for n in range(WIN // RADIUS)], axis=0
                )

            waiting.append((part(1), [(u, 0, 0)]))
            n = u % PACK
            edge = pltpu.roll(jnp.where(right_half, part(2), part(0)), turn(n), 1)
            packed = jnp.where(quarter == n, edge, packed) if n else edge
            if n == PACK - 1:
                uses = [(u - n + m, BS, (BS - turn(m)) % BS) for m in range(PACK)]
                waiting.append((packed, uses))
            while len(waiting) > 1:
                first_filter(*zip(waiting.pop(0), waiting.pop(0)))
        got = jnp.dot(along_rows[...], w_col[...], preferred_element_type=jnp.float32)
        filtered = got[:, :BS] + got[:, BS:]
        value = lower + jnp.tanh(SHARPNESS * (filtered - THRESHOLD))
        out = []
        for u, block in enumerate(blocks):
            scale = mask[block >> 5, block & (KC - 1)].astype(jnp.float32) * (1.0 / (lower + upper))
            out.append(scale * value[u * BS : (u + 1) * BS])
        return out

    def source_block(rank, target):
        pair = (table[rank, target * 2], table[rank, target * 2 + 1])
        return (jnp.minimum(*pair) if rank == 0 else jnp.maximum(*pair)) & (KR * KC - 1)

    def fill(g, half_x, half_y, acc):
        def step(half, n):
            return 3 - 3 * half if n else 1 + half

        places, blocks = [], []
        for u in range(BATCH):
            n, m, p = u // 8, u // SIDE % 2, u % SIDE
            to_x, to_y = (x + step(half_x, n)) & 3, (y + step(half_y, m)) & 3
            to_z = (z + STEPS[p]) & 3
            target = (to_y * 2 + ((core + g) & 1)) * 16 + to_x * SIDE + to_z
            blocks.append(source_block(g // 2, target))
            places.append((g, 2 * half_x + n, 2 * half_y + m, p))
        for place, value in zip(places, batch(blocks)):
            send[place] = value.astype(jnp.bfloat16)
            acc = acc + jnp.sum(value.reshape(BS // 8, 8, BS), axis=0)
        return acc

    def view(ref, g, picks, begin, rows):
        index = [picks.get(d, slice(None)) for d in range(3)]
        return ref.at[(g, *index, pl.ds(begin, rows), slice(None))]

    def remote(src, dst, axis, step, flip, sem):
        pltpu.make_async_remote_copy(
            src_ref=src, dst_ref=dst, send_sem=out_send.at[sem], recv_sem=out_recv.at[sem],
            device_id=device(along(axis, step), lax.rem(core + flip, 2)), device_id_type=MESH,
        ).start()

    def wait(sem, ref):
        pltpu.make_async_copy(ref, ref, sem).wait()

    def hop1(j, half_x=None, half_y=None):
        g, flip, (a, b, c), begin, rows = CHUNKS[j]
        for p in range(SIDE if flip else HOME):
            picks = {}
            for axis, half in ((0, half_x), (1, half_y)):
                if half is not None:
                    picks[axis] = pl.ds(2 * half, 2)
                    if axis == a and p // 2 != half:
                        break
            else:
                picks[a] = p
                remote(
                    view(send, g, picks, begin, rows), view(mid1, g, picks, begin, rows),
                    a, STEPS[p], flip, j,
                )

    def got1(j):
        g, flip, (a, b, c), begin, rows = CHUNKS[j]
        return view(mid1, g, {} if flip else {a: OTHERS}, begin, rows)

    def hop2(j):
        g, flip, (a, b, c), begin, rows = CHUNKS[j]
        wait(out_recv.at[j], got1(j))
        for p in range(HOME):
            if flip:
                pairs = ((mid1, {b: p}),)
            else:
                pairs = ((mid1, {b: p, a: OTHERS}), (send, {b: p, a: HOME}))
            for ref, picks in pairs:
                remote(
                    view(ref, g, picks, begin, rows), view(mid2, g, picks, begin, rows),
                    b, STEPS[p], 0, NCH + j,
                )

    def got2(j):
        g, flip, (a, b, c), begin, rows = CHUNKS[j]
        return view(mid2, g, {b: OTHERS}, begin, rows)

    def hop3(j):
        g, flip, (a, b, c), begin, rows = CHUNKS[j]
        wait(out_recv.at[NCH + j], got2(j))
        for p in range(SIDE):
            pairs = [(mid2, {c: p, b: OTHERS})]
            if flip:
                pairs.append((mid1, {c: p, b: HOME}))
            else:
                pairs.append((mid1, {c: p, b: HOME, a: OTHERS}))
                pairs.append((send, {c: p, b: HOME, a: HOME}))
            for ref, picks in pairs:
                src, dst = view(ref, g, picks, begin, rows), view(arrived, g, picks, begin, rows)
                if p != HOME:
                    remote(src, dst, c, STEPS[p], 0, 2 * NCH + j)
                else:
                    pltpu.make_async_copy(src, dst, local_sem.at[0]).start()

    def got3(j):
        g, flip, (a, b, c), begin, rows = CHUNKS[j]
        return view(arrived, g, {c: OTHERS}, begin, rows)

    def of(g):
        return range(3 * g, 3 * g + 3)

    volume = jnp.zeros((8, BS), jnp.float32)
    for g in range(GROUPS):
        if g < 2:
            for half_x in range(2):
                for half_y in range(2):
                    volume = fill(g, half_x, half_y, volume)
                    for j in of(g):
                        hop1(j, half_x, half_y)
                if g == 1 and half_x == 0:
                    for j in of(0):
                        hop2(j)
        else:
            volume = lax.fori_loop(
                0, SIDE, lambda n, acc, g=g: fill(g, n // 2, lax.rem(n, 2), acc), volume
            )
            for j in of(g):
                hop1(j)
            for j in of(g - 1):
                hop2(j)

    def spread(stage, own, slots, targets):
        first_slot = (0, 8, 12)[stage]
        sums[first_slot + own] = volume_parts[stage]
        for target in targets:
            pltpu.make_async_remote_copy(
                src_ref=sums.at[first_slot + own], dst_ref=sums.at[first_slot + own],
                send_sem=sum_send.at[stage], recv_sem=sum_recv.at[stage],
                device_id=target, device_id_type=MESH,
            ).start()

    def collect(stage, slots):
        first_slot = (0, 8, 12)[stage]
        for sem in (sum_recv, sum_send):
            wait(sem.at[stage], sums.at[pl.ds(first_slot, slots - 1)])
        out = sums[first_slot]
        for s in range(1, slots):
            out = out + sums[first_slot + s]
        return out

    volume_parts = [volume]
    spread(
        0, x * 2 + core, 8,
        [device(along(0, s), lax.rem(core + k, 2)) for s in range(SIDE) for k in range(2) if s or k],
    )
    for j in range(NCH - 3, NCH):
        hop2(j)
    volume_parts.append(collect(0, 8))
    spread(1, y, 4, [device(along(1, s), core) for s in range(1, SIDE)])
    for j in range(NCH):
        hop3(j)
    volume_parts.append(collect(1, 4))
    spread(2, z, 4, [device(along(2, s), core) for s in range(1, SIDE)])
    all_volume = jnp.sum(collect(2, 4))
    cells = float(ROWS * COLS * 128)
    constraint = all_volume / cells / VOLUME_TARGET - 1.0
    total[...] = jnp.full((8, BS), constraint, jnp.float32)

    for j in range(NCH):
        wait(out_recv.at[2 * NCH + j], got3(j))
    for j in range(NCH):
        wait(out_send.at[j], got1(j))
        wait(out_send.at[NCH + j], got2(j))
        wait(out_send.at[2 * NCH + j], got3(j))
        g, flip, (a, b, c), begin, rows = CHUNKS[j]
        wait(local_sem.at[0], view(arrived, g, {c: HOME}, begin, rows))
    for copy in halo:
        copy.wait_send()


def place_kernel(slots, total, arrived, out, constraint, sem):
    row = lax.axis_index("row")
    col = lax.axis_index("col")
    y, core, x, z = row // 2, row % 2, col // SIDE, col % SIDE

    from_x = [((x - step) & 3) * SIDE for step in STEPS]
    from_y = [((y - step) & 3) * 32 for step in STEPS]
    from_z = [(z - step) & 3 for step in STEPS]
    from_core = [((core + flip) & 1) * 16 for flip in range(2)]
    for g in range(GROUPS):
        for n in range(SIDE):
            for m in range(SIDE):
                base = from_core[g % 2] + from_x[n] + from_y[m]
                for p in range(SIDE):
                    pltpu.make_async_copy(
                        arrived.at[g, n, m, p], out.at[slots[g // 2, base + from_z[p]]], sem.at[0]
                    ).start()
    constraint[0, 0] = total[0, 0]
    pltpu.make_async_copy(out, out, sem.at[0]).wait()


def per_device(density, design_mask, rebalance):
    smem = pl.BlockSpec(memory_space=pltpu.SMEM)
    vmem = pl.BlockSpec(memory_space=pltpu.VMEM)
    anywhere = pl.BlockSpec(memory_space=pl.ANY)
    exchange = (GROUPS, SIDE, SIDE, SIDE, BS, BS)
    w_row, w_col = row_weights(), col_weights()
    dma = pltpu.SemaphoreType.DMA
    arrived, slots, total = pl.pallas_call(
        fused_kernel,
        out_shape=(
            pltpu.VMEM(exchange, jnp.bfloat16),
            pltpu.VMEM((8, BS), jnp.int32),
            pltpu.VMEM((8, BS), jnp.float32),
        ),
        in_specs=[anywhere, anywhere, anywhere, anywhere, smem],
        out_specs=(vmem, vmem, vmem),
        scratch_shapes=[
            pltpu.VMEM((KC + 2, GROUPS_IN + 2, RADIUS, BS), jnp.float32),
            pltpu.VMEM((2, RADIUS, COLS + 2 * BS), jnp.float32),
            pltpu.VMEM((BATCH * BS, 4 * BS), jnp.bfloat16),
            pltpu.VMEM((2 * BS, BS), jnp.int32),
            pltpu.VMEM(w_row.shape, jnp.bfloat16), pltpu.VMEM(w_col.shape, jnp.bfloat16),
            pltpu.VMEM((2, 2 * BS), jnp.int32), pltpu.SMEM((2, 2 * BS), jnp.int32),
            *[pltpu.VMEM(exchange, jnp.bfloat16)] * 3,
            pltpu.VMEM((2, BS, BS), jnp.float32), pltpu.VMEM((2, BS, BS), jnp.float32),
            pltpu.VMEM((16, 8, BS), jnp.float32),
            dma((KC,)), dma((3,)), dma((1,)), dma((8,)), dma((8,)), dma((3,)), dma((3,)),
            dma((3 * NCH,)), dma((3 * NCH,)), dma((1,)),
        ],
        compiler_params=pltpu.CompilerParams(
            collective_id=0, has_side_effects=True, vmem_limit_bytes=54 * 2**20
        ),
        name="filter_exchange",
    )(
        density.reshape(GROUPS_IN, RADIUS, COLS), rebalance.reshape(2 * BS, BS), jnp.asarray(w_row), jnp.asarray(w_col),
        design_mask,
    )
    balanced, constraint = pl.pallas_call(
        place_kernel,
        out_shape=(
            jax.ShapeDtypeStruct((KR * KC, BS, BS), jnp.bfloat16),
            jax.ShapeDtypeStruct((1, 1), jnp.float32),
        ),
        in_specs=[smem, smem, vmem],
        out_specs=(anywhere, smem),
        scratch_shapes=[dma((1,))],
        compiler_params=pltpu.CompilerParams(vmem_limit_bytes=10 * 2**20),
        name="place_blocks",
    )(slots, total, arrived)
    return balanced, constraint.reshape(())


def solution(mesh):
    return jax.shard_map(
        per_device, mesh=mesh,
        in_specs=(P("row", "col"), P("row", "col"), P()),
        out_specs=(P(("row", "col"), None, None), P()),
        check_vma=False,
    )
```

```python
import functools

import jax
import jax.numpy as jnp
import numpy as np
from jax import lax
from jax.experimental import pallas as pl
from jax.experimental.pallas import tpu as pltpu
from jax.sharding import PartitionSpec as P

BS = 128
RADIUS = 16
SHARPNESS = 32.0
THRESHOLD = 0.5
VOLUME_TARGET = 0.4
MESH = pl.DeviceIdType.MESH

KR = 8
KC = 32
SIDE = 4
GROUPS = 4
WIN = BS + 2 * RADIUS
ROWS = KR * BS
COLS = KC * BS
GROUPS_IN = ROWS // RADIUS
BATCH = 16
PACK = 4
STEPS = (1, 3, 2, 0)
OTHERS = pl.ds(0, SIDE - 1)
HOME = SIDE - 1

ROUTES = ((0, 1, 2), (1, 2, 0), (2, 0, 1))
PARTS = ((0, 48), (48, 48), (96, 32))
CHUNKS = tuple(
    (g, g % 2, ROUTES[i], *PARTS[(i + g) % 3]) for g in range(GROUPS) for i in range(3)
)
NCH = len(CHUNKS)


def filter_taps():
    sigma = RADIUS / 4.0
    offsets = np.arange(2 * RADIUS + 1, dtype=np.float64) - RADIUS
    raw = np.exp(-offsets * offsets / (2.0 * sigma * sigma))
    return raw / raw.sum()


def taps_at(lag):
    taps = filter_taps()
    inside = (lag >= 0) & (lag <= 2 * RADIUS)
    return np.where(inside, taps[np.clip(lag, 0, 2 * RADIUS)], 0.0).astype(np.float32)


def high_low(array):
    high = array.astype(jnp.bfloat16)
    low = (array - high.astype(np.float32)).astype(jnp.bfloat16)
    return high, low


def row_weights():
    lag = np.arange(WIN)[None, :] - np.arange(BS)[:, None]
    once = np.concatenate(high_low(taps_at(lag)), axis=0)
    return np.concatenate([once, once], axis=1)


def col_weights():
    lane = np.arange(BS)
    edge = np.where(lane < BS // 2, lane + BS, lane - BS)
    position = np.concatenate([lane, edge])
    lag = position[:, None] - lane[None, :] + RADIUS
    once = np.concatenate(high_low(taps_at(lag)), axis=1)
    return np.concatenate([once, once], axis=0)


def split_f32(value):
    high = value.astype(jnp.bfloat16)
    low = (value - high.astype(jnp.float32)).astype(jnp.bfloat16)
    return high, low


def fused_kernel(
    density, rebalance, w_row_in, w_col_in, mask,
    arrived, slots, total,
    field, rim, along_rows, ids, w_row, w_col, keys, table, send, mid1, mid2, edge_out, edge_in, sums,
    load_sem, aux_sem, table_sem, halo_send, halo_recv, sum_send, sum_recv,
    out_send, out_recv, local_sem,
):
    row = lax.axis_index("row")
    col = lax.axis_index("col")
    y, core = row // 2, row % 2
    x, z = col // SIDE, col % SIDE
    me = (x, y, z)
    my_id = row * 16 + col

    def device(c, k):
        return (c[1] * 2 + k, c[0] * SIDE + c[2])

    def along(axis, step):
        c = list(me)
        c[axis] = lax.rem(me[axis] + step, SIDE)
        return c

    inner = pl.ds(1, GROUPS_IN)
    aux = [
        pltpu.make_async_copy(src, dst, aux_sem.at[n])
        for n, (src, dst) in enumerate(((rebalance, ids), (w_row_in, w_row), (w_col_in, w_col)))
    ]
    loads = [
        pltpu.make_async_copy(
            density.at[:, :, pl.ds(tile * BS, BS)], field.at[tile + 1, inner], load_sem.at[min(n, 2)]
        )
        for n, tile in enumerate((0, KC - 1, *range(1, KC - 1)))
    ]
    edge_loads, loads = loads[:2], loads[2:]
    for copy in (*edge_loads, *aux, *loads):
        copy.start()

    next_row, prev_row = lax.rem(row + 1, 8), lax.rem(row + 7, 8)
    next_col, prev_col = lax.rem(col + 1, 16), lax.rem(col + 15, 16)
    greeted = [
        device(along(axis, step), lax.rem(core + k, 2))
        for axis in range(3) for step in range(1, SIDE) for k in range(2)
    ]
    greeted += [device(me, 1 - core), (row, next_col), (row, prev_col)]
    greeted += [(r, c) for r in (next_row, prev_row) for c in (next_col, prev_col)]
    barrier = pltpu.get_barrier_semaphore()
    for target in greeted:
        pl.semaphore_signal(barrier, inc=1, device_id=target, device_id_type=MESH)

    for copy in edge_loads:
        copy.wait()
    lane_group = lax.broadcasted_iota(jnp.int32, (BS, BS), 1) // RADIUS
    for side, (tile, first_lane) in enumerate(((0, 0), (KC - 1, BS - RADIUS))):
        packed = jnp.zeros((BS, BS), jnp.float32)
        for i in range(KR):
            value = field[tile + 1, pl.ds(1 + i * 8, 8)].reshape(BS, BS)
            moved = pltpu.roll(value, (RADIUS * i - first_lane) % BS, 1)
            packed = jnp.where(lane_group == i, moved, packed)
        edge_out[side] = packed

    pl.semaphore_wait(barrier, len(greeted))

    last = GROUPS_IN - 1
    own_left, own_right = pl.ds(0, BS), pl.ds(COLS - BS, BS)
    wide, left, right = pl.ds(BS, COLS), pl.ds(0, BS), pl.ds(BS + COLS, BS)
    halo = [
        (edge_out.at[0], edge_in.at[1], (row, prev_col)),
        (edge_out.at[1], edge_in.at[0], (row, next_col)),
        (density.at[last], rim.at[0, :, wide], (next_row, col)),
        (density.at[0], rim.at[1, :, wide], (prev_row, col)),
        (density.at[last, :, own_right], rim.at[0, :, left], (next_row, next_col)),
        (density.at[last, :, own_left], rim.at[0, :, right], (next_row, prev_col)),
        (density.at[0, :, own_right], rim.at[1, :, left], (prev_row, next_col)),
        (density.at[0, :, own_left], rim.at[1, :, right], (prev_row, prev_col)),
    ]
    halo = [
        pltpu.make_async_remote_copy(
            src_ref=src, dst_ref=dst, send_sem=halo_send.at[n], recv_sem=halo_recv.at[n],
            device_id=target, device_id_type=MESH,
        )
        for n, (src, dst, target) in enumerate(halo)
    ]
    for copy in halo:
        copy.start()

    for copy in aux:
        copy.wait()

    def owner(number):
        return (number >> 12) * 16 + ((number >> 5) & 15)

    def local(number):
        return ((number >> 9) & 7) * KC + (number & (KC - 1))

    none = 1 << 20
    turned = ids[...].T
    mine = owner(turned) == my_id
    block = local(turned)
    keys[pl.ds(0, 1), :] = jnp.min(jnp.where(mine, block, none), 0, keepdims=True)
    keys[pl.ds(1, 1), :] = jnp.max(jnp.where(mine, block, -1), 0, keepdims=True)
    to_table = pltpu.make_async_copy(keys, table, table_sem.at[0])
    to_table.start()
    low, high = jnp.full((1, BS), none, jnp.int32), jnp.full((1, BS), -1, jnp.int32)
    source = lax.broadcasted_iota(jnp.int32, (BS, BS), 1)
    for half in range(2):
        own = jnp.broadcast_to(ids[pl.ds(my_id * 2 + half, 1), :], (BS, BS)).T
        slot = lax.broadcasted_iota(jnp.int32, (BS, BS), 0) + half * BS
        key = local(own) * 256 + slot
        here = owner(own) == source
        low = jnp.minimum(low, jnp.min(jnp.where(here, key, none), 0, keepdims=True))
        high = jnp.maximum(high, jnp.max(jnp.where(here, key, -1), 0, keepdims=True))
    slots[...] = jnp.zeros_like(slots)
    slots[pl.ds(0, 1), :] = low & 255
    slots[pl.ds(1, 1), :] = high & 255

    for copy in halo:
        copy.wait_recv()
    bulk = field.at[pl.ds(2, KC - 2), inner]
    pltpu.make_async_copy(bulk, bulk, load_sem.at[2]).wait()

    def kept(condition):
        return jnp.where(condition, 1.0, 0.0).astype(jnp.float32)

    keep_side = (kept(col > 0), kept(col < 15))
    for side, (tile, first_lane) in enumerate(((0, BS - RADIUS), (KC + 1, 0))):
        value = edge_in[side] * keep_side[side]
        for i in range(KR):
            moved = pltpu.roll(value, (first_lane - RADIUS * i) % BS, 1)
            field[tile, pl.ds(1 + i * 8, 8)] = moved.reshape(8, RADIUS, BS)
    for end, (group, keep) in enumerate(((0, kept(row > 0)), (GROUPS_IN + 1, kept(row < 7)))):
        for tile in range(KC + 2):
            scale = keep * keep_side[tile > 0] if tile in (0, KC + 1) else keep
            field[tile, group] = rim[end, :, tile * BS : (tile + 1) * BS] * scale
    to_table.wait()

    right_half = lax.broadcasted_iota(jnp.int32, (WIN, BS), 1) < BS // 2
    quarter = lax.broadcasted_iota(jnp.int32, (WIN, BS), 1) // (2 * RADIUS)
    lower = float(np.tanh(np.float32(SHARPNESS * THRESHOLD)))
    upper = float(np.tanh(np.float32(SHARPNESS * (1.0 - THRESHOLD))))

    def turn(n):
        return 2 * RADIUS * n + RADIUS

    def first_filter(tiles, uses):
        window = jnp.concatenate(tiles, axis=1)
        got = jnp.dot(
            w_row[...], jnp.concatenate(split_f32(window), axis=0),
            preferred_element_type=jnp.float32,
        )
        got = got[:BS] + got[BS:]
        for n, tile_uses in enumerate(uses):
            for u, offset, shift in tile_uses:
                value = got[:, n * BS : (n + 1) * BS]
                if shift:
                    value = pltpu.roll(value, shift, 1)
                for m, piece in enumerate(split_f32(value)):
                    at = 2 * BS * m + offset
                    along_rows[u * BS : (u + 1) * BS, at : at + BS] = piece

    def batch(blocks):
        waiting = []
        packed = None
        for u, block in enumerate(blocks):
            tile = block & (KC - 1)
            group = (block >> 5) * 8

            def part(offset):
                return jnp.concatenate(
                    [field[tile + offset, group + n] for n in range(WIN // RADIUS)], axis=0
                )

            waiting.append((part(1), [(u, 0, 0)]))
            n = u % PACK
            edge = pltpu.roll(jnp.where(right_half, part(2), part(0)), turn(n), 1)
            packed = jnp.where(quarter == n, edge, packed) if n else edge
            if n == PACK - 1:
                uses = [(u - n + m, BS, (BS - turn(m)) % BS) for m in range(PACK)]
                waiting.append((packed, uses))
            while len(waiting) > 1:
                first_filter(*zip(waiting.pop(0), waiting.pop(0)))
        got = jnp.dot(along_rows[...], w_col[...], preferred_element_type=jnp.float32)
        filtered = got[:, :BS] + got[:, BS:]
        value = lower + jnp.tanh(SHARPNESS * (filtered - THRESHOLD))
        out = []
        for u, block in enumerate(blocks):
            scale = mask[block >> 5, block & (KC - 1)].astype(jnp.float32) * (1.0 / (lower + upper))
            out.append(scale * value[u * BS : (u + 1) * BS])
        return out

    def source_block(rank, target):
        pair = (table[rank, target * 2], table[rank, target * 2 + 1])
        return (jnp.minimum(*pair) if rank == 0 else jnp.maximum(*pair)) & (KR * KC - 1)

    def fill(g, half_x, half_y, acc):
        def step(half, n):
            return 3 - 3 * half if n else 1 + half

        places, blocks = [], []
        for u in range(BATCH):
            n, m, p = u // 8, u // SIDE % 2, u % SIDE
            to_x, to_y = (x + step(half_x, n)) & 3, (y + step(half_y, m)) & 3
            to_z = (z + STEPS[p]) & 3
            target = (to_y * 2 + ((core + g) & 1)) * 16 + to_x * SIDE + to_z
            blocks.append(source_block(g // 2, target))
            places.append((g, 2 * half_x + n, 2 * half_y + m, p))
        for place, value in zip(places, batch(blocks)):
            send[place] = value.astype(jnp.bfloat16)
            acc = acc + jnp.sum(value.reshape(BS // 8, 8, BS), axis=0)
        return acc

    def view(ref, g, picks, begin, rows):
        index = [picks.get(d, slice(None)) for d in range(3)]
        return ref.at[(g, *index, pl.ds(begin, rows), slice(None))]

    def remote(src, dst, axis, step, flip, sem):
        pltpu.make_async_remote_copy(
            src_ref=src, dst_ref=dst, send_sem=out_send.at[sem // NCH], recv_sem=out_recv.at[sem],
            device_id=device(along(axis, step), lax.rem(core + flip, 2)), device_id_type=MESH,
        ).start()

    def wait(sem, ref):
        pltpu.make_async_copy(ref, ref, sem).wait()

    def hop1(j, half_x=None, half_y=None):
        g, flip, (a, b, c), begin, rows = CHUNKS[j]
        for p in range(SIDE if flip else HOME):
            picks = {}
            for axis, half in ((0, half_x), (1, half_y)):
                if half is not None:
                    picks[axis] = pl.ds(2 * half, 2)
                    if axis == a and p // 2 != half:
                        break
            else:
                picks[a] = p
                remote(
                    view(send, g, picks, begin, rows), view(mid1, g, picks, begin, rows),
                    a, STEPS[p], flip, j,
                )

    def got1(j):
        g, flip, (a, b, c), begin, rows = CHUNKS[j]
        return view(mid1, g, {} if flip else {a: OTHERS}, begin, rows)

    def hop2(j):
        g, flip, (a, b, c), begin, rows = CHUNKS[j]
        wait(out_recv.at[j], got1(j))
        for p in range(HOME):
            if flip:
                pairs = ((mid1, {b: p}),)
            else:
                pairs = ((mid1, {b: p, a: OTHERS}), (send, {b: p, a: HOME}))
            for ref, picks in pairs:
                remote(
                    view(ref, g, picks, begin, rows), view(mid2, g, picks, begin, rows),
                    b, STEPS[p], 0, NCH + j,
                )

    def got2(j):
        g, flip, (a, b, c), begin, rows = CHUNKS[j]
        return view(mid2, g, {b: OTHERS}, begin, rows)

    def hop3(j):
        g, flip, (a, b, c), begin, rows = CHUNKS[j]
        wait(out_recv.at[NCH + j], got2(j))
        for p in range(SIDE):
            pairs = [(mid2, {c: p, b: OTHERS})]
            if flip:
                pairs.append((mid1, {c: p, b: HOME}))
            else:
                pairs.append((mid1, {c: p, b: HOME, a: OTHERS}))
                pairs.append((send, {c: p, b: HOME, a: HOME}))
            for ref, picks in pairs:
                src, dst = view(ref, g, picks, begin, rows), view(arrived, g, picks, begin, rows)
                if p != HOME:
                    remote(src, dst, c, STEPS[p], 0, 2 * NCH + j)
                else:
                    pltpu.make_async_copy(src, dst, local_sem.at[0]).start()

    def got3(j):
        g, flip, (a, b, c), begin, rows = CHUNKS[j]
        return view(arrived, g, {c: OTHERS}, begin, rows)

    def of(g):
        return range(3 * g, 3 * g + 3)

    def spread(stage, own, slots, targets):
        first_slot = (0, 8, 12)[stage]
        sums[first_slot + own] = volume_parts[stage]
        for target in targets:
            pltpu.make_async_remote_copy(
                src_ref=sums.at[first_slot + own], dst_ref=sums.at[first_slot + own],
                send_sem=sum_send.at[stage], recv_sem=sum_recv.at[stage],
                device_id=target, device_id_type=MESH,
            ).start()

    def collect(stage, slots):
        first_slot = (0, 8, 12)[stage]
        for sem in (sum_recv, sum_send):
            wait(sem.at[stage], sums.at[pl.ds(first_slot, slots - 1)])
        out = sums[first_slot]
        for s in range(1, slots):
            out = out + sums[first_slot + s]
        return out

    volume = jnp.zeros((8, BS), jnp.float32)
    for g in range(GROUPS):
        if g < 2:
            for half_x in range(2):
                for half_y in range(2):
                    volume = fill(g, half_x, half_y, volume)
                    for j in of(g):
                        hop1(j, half_x, half_y)
                if g == 1 and half_x == 0:
                    for j in of(0):
                        hop2(j)
        else:
            volume = lax.fori_loop(
                0, SIDE, lambda n, acc, g=g: fill(g, n // 2, lax.rem(n, 2), acc), volume
            )
            if g == GROUPS - 1:
                volume_parts = [volume]
                spread(
                    0, x * 2 + core, 8,
                    [
                        device(along(0, s), lax.rem(core + k, 2))
                        for s in range(SIDE) for k in range(2) if s or k
                    ],
                )
            for j in of(g):
                hop1(j)
            for j in of(g - 1):
                hop2(j)

    volume_parts.append(collect(0, 8))
    spread(1, y, 4, [device(along(1, s), core) for s in range(1, SIDE)])
    for j in of(GROUPS - 1):
        hop2(j)
    for j in range(NCH - 3):
        hop3(j)
    volume_parts.append(collect(1, 4))
    spread(2, z, 4, [device(along(2, s), core) for s in range(1, SIDE)])
    for j in of(GROUPS - 1):
        hop3(j)
    all_volume = jnp.sum(collect(2, 4))
    cells = float(ROWS * COLS * 128)
    constraint = all_volume / cells / VOLUME_TARGET - 1.0
    total[...] = jnp.full((8, BS), constraint, jnp.float32)

    for j in range(NCH):
        wait(out_recv.at[2 * NCH + j], got3(j))
    wait(out_send.at[0], mid1.at[:, :, :, :, pl.ds(0, BS * 7 // 8)])
    wait(out_send.at[1], mid2.at[:, OTHERS])
    wait(out_send.at[2], arrived.at[:, OTHERS])
    wait(local_sem.at[0], arrived.at[:, HOME])
    for copy in halo:
        copy.wait_send()


def place_kernel(slots, total, arrived, out, constraint, sem):
    row = lax.axis_index("row")
    col = lax.axis_index("col")
    y, core, x, z = row // 2, row % 2, col // SIDE, col % SIDE

    from_x = [((x - step) & 3) * SIDE for step in STEPS]
    from_y = [((y - step) & 3) * 32 for step in STEPS]
    from_z = [(z - step) & 3 for step in STEPS]
    from_core = [((core + flip) & 1) * 16 for flip in range(2)]
    for g in range(GROUPS):
        for n in range(SIDE):
            for m in range(SIDE):
                base = from_core[g % 2] + from_x[n] + from_y[m]
                for p in range(SIDE):
                    pltpu.make_async_copy(
                        arrived.at[g, n, m, p], out.at[slots[g // 2, base + from_z[p]]], sem.at[0]
                    ).start()
    constraint[0, 0] = total[0, 0]
    pltpu.make_async_copy(out, out, sem.at[0]).wait()


def per_device(density, design_mask, rebalance):
    smem = pl.BlockSpec(memory_space=pltpu.SMEM)
    vmem = pl.BlockSpec(memory_space=pltpu.VMEM)
    anywhere = pl.BlockSpec(memory_space=pl.ANY)
    exchange = (GROUPS, SIDE, SIDE, SIDE, BS, BS)
    w_row, w_col = row_weights(), col_weights()
    dma = pltpu.SemaphoreType.DMA
    arrived, slots, total = pl.pallas_call(
        fused_kernel,
        out_shape=(
            pltpu.VMEM(exchange, jnp.bfloat16),
            pltpu.VMEM((8, BS), jnp.int32),
            pltpu.VMEM((8, BS), jnp.float32),
        ),
        in_specs=[anywhere, anywhere, anywhere, anywhere, smem],
        out_specs=(vmem, vmem, vmem),
        scratch_shapes=[
            pltpu.VMEM((KC + 2, GROUPS_IN + 2, RADIUS, BS), jnp.float32),
            pltpu.VMEM((2, RADIUS, COLS + 2 * BS), jnp.float32),
            pltpu.VMEM((BATCH * BS, 4 * BS), jnp.bfloat16),
            pltpu.VMEM((2 * BS, BS), jnp.int32),
            pltpu.VMEM(w_row.shape, jnp.bfloat16), pltpu.VMEM(w_col.shape, jnp.bfloat16),
            pltpu.VMEM((2, 2 * BS), jnp.int32), pltpu.SMEM((2, 2 * BS), jnp.int32),
            *[pltpu.VMEM(exchange, jnp.bfloat16)] * 3,
            pltpu.VMEM((2, BS, BS), jnp.float32), pltpu.VMEM((2, BS, BS), jnp.float32),
            pltpu.VMEM((16, 8, BS), jnp.float32),
            dma((3,)), dma((3,)), dma((1,)), dma((8,)), dma((8,)), dma((3,)), dma((3,)),
            dma((3,)), dma((3 * NCH,)), dma((1,)),
        ],
        compiler_params=pltpu.CompilerParams(
            collective_id=0, has_side_effects=True, vmem_limit_bytes=54 * 2**20
        ),
        name="filter_exchange",
    )(
        density.reshape(GROUPS_IN, RADIUS, COLS), rebalance.reshape(2 * BS, BS), jnp.asarray(w_row), jnp.asarray(w_col),
        design_mask,
    )
    balanced, constraint = pl.pallas_call(
        place_kernel,
        out_shape=(
            jax.ShapeDtypeStruct((KR * KC, BS, BS), jnp.bfloat16),
            jax.ShapeDtypeStruct((1, 1), jnp.float32),
        ),
        in_specs=[smem, smem, vmem],
        out_specs=(anywhere, smem),
        scratch_shapes=[dma((1,))],
        compiler_params=pltpu.CompilerParams(vmem_limit_bytes=10 * 2**20),
        name="place_blocks",
    )(slots, total, arrived)
    return balanced, constraint.reshape(())


def solution(mesh):
    return jax.shard_map(
        per_device, mesh=mesh,
        in_specs=(P("row", "col"), P("row", "col"), P()),
        out_specs=(P(("row", "col"), None, None), P()),
        check_vma=False,
    )
```
